256 devices in a mesh: group: 64 (over z, y, core), section: 4 (over x).
Axes of the slice: x: 4, y: 4, z: 8, core: 2. Of those that a mesh axis runs over, the one named last changes fastest.
Arguments:
- embed_in: bfloat16 [256, 32, 1792], P(('group', 'section')), may hold values from -6 to 6
- clean_cache: bfloat16 [4, 256, 32, 1792], P('section', 'group'), may hold values from -6 to 6
- lengths: int32 [256, 5], P(('group', 'section')), may hold values from 1 to 24, 32 in all within a row
- patch_layer: int32 [256, 4], P(('group', 'section')), may hold values from 0 to 3
- patch_pos: int32 [256, 4], P(('group', 'section')), may hold values from 0 to 31
- answers: int32 [256, 4, 2], P(('group', 'section')), may hold values from 0 to 77823
- attn_gain: float32 [4, 1792], P('section'), may hold values from 0.5 to 1.5
- w_query: bfloat16 [4, 1792, 1792], P('section', 'group'), may hold values from -0.125 to 0.125
- b_query: float32 [4, 1792], P('section'), may hold values from -3 to 3
- w_keyval: bfloat16 [4, 1792, 512], P('section', 'group'), may hold values from -0.125 to 0.125
- b_key: float32 [4, 256], P('section'), may hold values from -3 to 3
- b_value: float32 [4, 256], P('section'), may hold values from -3 to 3
- w_out: bfloat16 [4, 1792, 1792], P('section', 'group'), may hold values from -0.125 to 0.125
- final_gain: float32 [1792], replicated, may hold values from 0.5 to 1.5
- unembed: bfloat16 [77824, 1792], P(('group', 'section')), may hold values from -0.125 to 0.125
Outputs:
- final_resid: bfloat16 [256, 32, 1792], P(('group', 'section'))
- logit_diff: float32 [256, 4], P(('group', 'section'))
- cell_sums: float32 [4, 24], replicated
The draws below stay inside these ranges and needn't reach their ends.
Inputs may be any that keep to these rules, and one draw needn't show every extreme that they name: Each row holds 4 prompt lengths followed by the padding of its bucket and sums to 32.
All inputs are finite; a program needn't handle non-finite values.
Results may differ from the reference program's by a relative error of at most 0.02.
Values may be sent and summed in bfloat16 or wider, within the bound.
No kernel may reach another device: no remote copies, remote signals or barrier semaphores. Data moves between devices by JAX's collectives and lax.ppermute only.
A program may use at most 128 MiB of HBM per device.

```python
import math
import jax
import jax.numpy as jnp
import numpy as np
from jax import lax

D = 1792
HQ = 14
KV = 2
HD = 128
VOCAB = 77824
L = 32
PB = 4
MAXLEN = 24
NB = 256
N_SECTION = 4


def plant(values, stream_key, low, largest):
    dims = values.shape
    index_at = [jax.random.randint(jax.random.fold_in(stream_key, axis), (), 0, dims[axis]) for axis in range(len(dims))]
    values = values.at[tuple(index_at)].set(low)
    longest = dims.index(max(dims))
    index_at[longest] = (index_at[longest] + 1) % dims[longest]
    return values.at[tuple(index_at)].set(largest)


def block_levels(own_key, extent, pieces, smallest, largest):
    gain, own = 1.0, jax.random.fold_in(own_key, 6)
    for dim, parts in pieces:
        heights = jnp.exp(jax.random.uniform(jax.random.fold_in(own, dim), (parts,), jnp.float32, smallest / len(pieces), largest / len(pieces)))
        gain = gain * jnp.repeat(heights, extent[dim] // parts).reshape([-1 if axis == dim else 1 for axis in range(len(extent))])
    return gain


def length_profile(number_of, total, bound, skew):
    loads = [(1 << 20) // math.isqrt(rank ** skew) + 1 for rank in range(2, number_of + 1)]
    surplus, counts = total - bound - (number_of - 1), [1] * (number_of - 1)
    while surplus > 0:
        free = [i for i in range(number_of - 1) if counts[i] < bound]
        whole, remaining = sum([loads[i] for i in free]), surplus
        for i in free:
            extra = min(bound - counts[i], max(1, remaining * loads[i] // whole), surplus)
            counts[i] = counts[i] + extra
            surplus = surplus - extra
    return np.array([bound] + counts)


def ragged_sizes(key, number_of, total, limit, skew):
    if number_of == 2:
        one = jax.random.randint(key, (), max(1, total - limit), min(limit, total - 1) + 1)
        return jnp.stack([one, total - one])
    tallies = jnp.asarray(length_profile(number_of, total, limit, skew), jnp.int32)
    couples = (number_of - 1) // 2
    donor, receiver = tallies[1:1 + 2 * couples:2], tallies[2:2 + 2 * couples:2]
    slack = jnp.minimum(donor - 1, limit - receiver)
    passed = jax.random.randint(jax.random.fold_in(key, 1), (couples,), 0, 1 << 20) % (slack + 1)
    tallies = tallies.at[1:1 + 2 * couples:2].set(donor - passed).at[2:2 + 2 * couples:2].set(receiver + passed)
    return tallies[jax.random.permutation(jax.random.fold_in(key, 2), number_of)]


def centred(rng, extent, deviation, limit, split=(), kind=jnp.bfloat16):
    factor_of = block_levels(rng, extent, split, -0.22, 0.18) if split else 1.0
    entries = jax.random.normal(rng, extent, jnp.float32) * deviation * factor_of
    return jnp.minimum(jnp.maximum(entries, -limit), limit).astype(kind)


def setup_inputs(seed: int = 0) -> dict:
    arg_keys = jax.random.split(jax.random.key(seed), 16)
    return {
        "embed_in": centred(arg_keys[0], (NB, L, D), 1.0, 6.0, ((0, 256),)),
        "clean_cache": centred(arg_keys[1], (N_SECTION, NB, L, D), 1.0, 6.0, ((0, 4), (1, 64))),
        "lengths": jax.vmap(lambda own: ragged_sizes(own, PB + 1, L, MAXLEN, 2))(jax.random.split(arg_keys[2], NB)).reshape((NB, PB + 1)).astype(jnp.int32),
        "patch_layer": plant(jax.random.randint(arg_keys[3], (NB, PB), 0, N_SECTION), jax.random.fold_in(arg_keys[3], 1), 0, N_SECTION - 1).astype(jnp.int32),
        "patch_pos": plant(jax.random.randint(arg_keys[4], (NB, PB), 0, L), jax.random.fold_in(arg_keys[4], 1), 0, L - 1).astype(jnp.int32),
        "answers": plant(jax.random.randint(arg_keys[5], (NB, PB, 2), 0, VOCAB), jax.random.fold_in(arg_keys[5], 1), 0, VOCAB - 1).astype(jnp.int32),
        "attn_gain": jnp.clip(1.0 + 0.1 * jax.random.normal(arg_keys[6], (N_SECTION, D), jnp.float32), 0.5, 1.5),
        "w_query": centred(arg_keys[7], (N_SECTION, D, HQ * HD), D ** -0.5, 0.125, ((0, 4), (1, 64))),
        "b_query": centred(arg_keys[8], (N_SECTION, HQ * HD), 0.5, 3.0, ((0, 4),), jnp.float32),
        "w_keyval": centred(arg_keys[9], (N_SECTION, D, 2 * KV * HD), D ** -0.5, 0.125, ((0, 4), (1, 64))),
        "b_key": centred(arg_keys[10], (N_SECTION, KV * HD), 0.5, 3.0, ((0, 4),), jnp.float32),
        "b_value": centred(arg_keys[11], (N_SECTION, KV * HD), 0.5, 3.0, ((0, 4),), jnp.float32),
        "w_out": centred(arg_keys[12], (N_SECTION, HQ * HD, D), (HQ * HD) ** -0.5, 0.125, ((0, 4), (1, 64))),
        "final_gain": jnp.clip(1.0 + 0.1 * jax.random.normal(arg_keys[13], (D,), jnp.float32), 0.5, 1.5),
        "unembed": centred(arg_keys[14], (VOCAB, D), D ** -0.5, 0.125, ((0, 256),)),
    }


epsilon = 1e-06
rope_base = 1000000.0

def rmsnorm(hidden, norm_gain):
    residual = hidden.astype(jnp.float32)
    scaled = residual * lax.rsqrt(lax.optimization_barrier(jnp.mean(residual * residual, axis=-1, keepdims=True)) + epsilon)
    return (scaled * norm_gain).astype(jnp.bfloat16)

def rotary(heads, position):
    half_dim = heads.shape[-1] // 2
    frequency = jnp.exp(jnp.arange(half_dim, dtype=jnp.float32) * (-math.log(rope_base) / half_dim))
    angles = position.astype(jnp.float32)[:, None] * frequency[None, :]
    cosine = jnp.cos(angles)[:, None, :]
    sinus = jnp.sin(angles)[:, None, :]
    front_half = heads[..., :half_dim]
    back_half = heads[..., half_dim:]
    return jnp.concatenate([front_half * cosine - back_half * sinus, back_half * cosine + front_half * sinus], axis=-1)

def bucket_layout(lengths_rows, seq_len):
    end_rows = jnp.cumsum(lengths_rows, axis=-1).astype(jnp.int32)
    starts = (end_rows - lengths_rows).astype(jnp.int32)
    row_ids = jnp.arange(seq_len, dtype=jnp.int32)
    segment = lax.optimization_barrier(jnp.sum((row_ids[:, None] >= end_rows[..., None, :]).astype(jnp.int32), axis=-1)).astype(jnp.int32)
    slots = jnp.arange(lengths_rows.shape[-1], dtype=jnp.int32)
    member = segment[..., :, None] == slots
    position = (row_ids - lax.optimization_barrier(jnp.sum(jnp.where(member, starts[..., None, :], 0), axis=-1))).astype(jnp.int32)
    return (segment, position, starts)

def patch_hits(starts, lengths_rows, layers, offsets, layer_now, seq_len):
    prompts = layers.shape[-1]
    target = (starts[..., :prompts] + offsets % lengths_rows[..., :prompts]).astype(jnp.int32)
    row_ids = jnp.arange(seq_len, dtype=jnp.int32)
    return jnp.any((row_ids[:, None] == target[..., None, :]) & (layers[..., None, :] == layer_now), axis=-1)

def attention_layer(hidden, norm_gain, query_weight, query_bias, keyval_weight, key_bias, value_bias, output_weight, segment, position):
    count_rows = hidden.shape[0]
    normed = rmsnorm(hidden, norm_gain)
    queries = jnp.dot(normed, query_weight, preferred_element_type=jnp.float32) + query_bias
    keyval = jnp.dot(normed, keyval_weight, preferred_element_type=jnp.float32)
    width_kv = keyval.shape[1] // 2
    keys_rot = rotary((keyval[:, :width_kv] + key_bias).reshape(count_rows, KV, HD), position).astype(jnp.bfloat16)
    values_all = (keyval[:, width_kv:] + value_bias).reshape(count_rows, KV, HD).astype(jnp.bfloat16)
    queries_rot = rotary(queries.reshape(count_rows, HQ, HD), position).astype(jnp.bfloat16)
    queries_rot = queries_rot.reshape(count_rows, KV, HQ // KV, HD)
    scores = jnp.einsum('qgrd,kgd->grqk', queries_rot.astype(jnp.float32), keys_rot.astype(jnp.float32)) * HD ** (-0.5)
    row_ids = jnp.arange(count_rows, dtype=jnp.int32)
    allowed = (segment[:, None] == segment[None, :]) & (row_ids[None, :] <= row_ids[:, None])
    scores = jnp.where(allowed, scores, -1e+30)
    weights = jax.nn.softmax(scores, axis=-1).astype(jnp.bfloat16)
    attended = jnp.einsum('grqk,kgd->qgrd', weights.astype(jnp.float32), values_all.astype(jnp.float32))
    attended = attended.astype(jnp.bfloat16).reshape(count_rows, HQ * HD)
    updated = hidden.astype(jnp.float32) + jnp.dot(attended, output_weight, preferred_element_type=jnp.float32)
    return updated.astype(jnp.bfloat16)

def reference(embed_in, clean_cache, lengths, patch_layer, patch_pos, answers, attn_gain, w_query, b_query, w_keyval, b_key, b_value, w_out, final_gain, unembed):
    segment, position, starts = bucket_layout(lengths, L)

    def one_bucket(items):
        hidden, clean, seg_row, pos_row, start_row, length_row, layer_row, offset_row = items
        for layer_now in range(N_SECTION):
            patched = patch_hits(start_row, length_row, layer_row, offset_row, layer_now, L)
            hidden = jnp.where(patched[:, None], clean[layer_now], hidden)
            hidden = attention_layer(hidden, attn_gain[layer_now], w_query[layer_now], b_query[layer_now], w_keyval[layer_now], b_key[layer_now], b_value[layer_now], w_out[layer_now], seg_row, pos_row)
        return hidden
    final_resid = lax.map(one_bucket, (embed_in, jnp.swapaxes(clean_cache, 0, 1), segment, position, starts, lengths, patch_layer, patch_pos))
    prompts = patch_layer.shape[1]
    last_rows = (starts[:, :prompts] + lengths[:, :prompts] - 1).astype(jnp.int32)
    picked = jnp.take_along_axis(final_resid, last_rows[:, :, None], axis=1)
    readout = rmsnorm(picked, final_gain).astype(jnp.float32)
    right_rows = unembed[answers[..., 0]].astype(jnp.float32)
    wrong_rows = unembed[answers[..., 1]].astype(jnp.float32)
    logit_diff = lax.optimization_barrier(jnp.sum(readout * right_rows, axis=-1)) - lax.optimization_barrier(jnp.sum(readout * wrong_rows, axis=-1))
    offsets = lengths[:, :prompts] - 1 - patch_pos % lengths[:, :prompts]
    cell_ids = (patch_layer * MAXLEN + offsets).astype(jnp.int32).reshape(-1)
    onehot = (cell_ids[:, None] == jnp.arange(N_SECTION * MAXLEN, dtype=jnp.int32)[None, :]).astype(jnp.float32)
    cell_sums = jnp.dot(logit_diff.reshape(-1), onehot, precision=lax.Precision.HIGHEST).reshape(N_SECTION, MAXLEN)
    return (final_resid, logit_diff, cell_sums)
```

```python
import functools
import math

import jax
import jax.numpy as jnp
from jax import lax
from jax.experimental import pallas as pl
from jax.experimental.pallas import tpu as pltpu
from jax.sharding import Mesh
from jax.sharding import PartitionSpec as P

HQ = 14
KV = 2
HD = 128
MAXLEN = 24
GROUP = ("group_0", "group_1", "group_2")
GROUP_SECTION = ("group_0", "group_1", "group_2", "section")

epsilon = 1e-06
rope_base = 1000000.0


def shifted(block, axis, distance):
    count = lax.axis_size(axis)
    return lax.ppermute(block, axis, [(i, (i + distance) % count) for i in range(count)])


def ring_gather(block, axis, halved):
    count = lax.axis_size(axis)
    pieces = [(0, 0, block)]
    right = left = block
    for step in range(1, count // 2):
        right = shifted(right, axis, 1)
        left = shifted(left, axis, -1)
        pieces += [(-step, 0, right), (step, 0, left)]
    width = block.shape[halved] // 2
    near = lax.slice_in_dim(right, 0, width, axis=halved)
    far = lax.slice_in_dim(left, width, 2 * width, axis=halved)
    pieces.append((count // 2, 0, shifted(near, axis, 1)))
    pieces.append((count // 2, width, shifted(far, axis, -1)))
    return pieces


def stacked(pieces, halved):
    count = max(offset for offset, _, _ in pieces) * 2
    by_offset = {}
    for offset, first, block in pieces:
        by_offset.setdefault(offset % count, []).append((first, block))
    rows = []
    for offset in range(count):
        parts = [block for _, block in sorted(by_offset[offset], key=lambda entry: entry[0])]
        rows.append(parts[0] if len(parts) == 1 else jnp.concatenate(parts, axis=halved))
    return jnp.stack(rows)


def swap_cores(block):
    return lax.ppermute(block, "group_2", [(0, 1), (1, 0)])


def gather_section(own_block):
    width = own_block.shape[1] // 2
    across_y = stacked(ring_gather(own_block[:, :width], "group_1", 1), 1)
    across_z = stacked(ring_gather(own_block[:, width:], "group_0", 1), 1)
    found = []
    for offset, first, block in ring_gather(across_y, "group_0", 2):
        found.append((True, offset, first, block))
    for offset, first, block in ring_gather(across_z, "group_1", 2):
        found.append((False, offset, width + first, block))
    return found


def place_kernel(plan, place_ref, *refs):
    blocks, out_ref, sems = refs[: len(plan)], refs[-2], refs[-1]
    z, y, core = place_ref[0], place_ref[1], place_ref[2]
    copies = []
    for (mine, y_first, offset, first), block in zip(plan, blocks):
        half = core if mine else 1 - core
        columns = block.shape[2]
        for inner in range(block.shape[0]):
            if y_first:
                chip = (z + offset + 8) % 8 * 4 + (y + inner) % 4
            else:
                chip = (z + inner) % 8 * 4 + (y + offset + 4) % 4
            rows = pl.ds(pl.multiple_of(chip * 56, 8), 56)
            copies.append(
                pltpu.make_async_copy(
                    block.at[inner],
                    out_ref.at[half, rows, pl.ds(first, columns)],
                    sems.at[len(copies)],
                )
            )
    for copy in copies:
        copy.start()
    for copy in copies:
        copy.wait()


def placed(own_pieces, partner_pieces, place, rows, columns):
    plan = [(True, *entry[:3]) for entry in own_pieces]
    plan += [(False, *entry[:3]) for entry in partner_pieces]
    blocks = [entry[3] for entry in own_pieces] + [entry[3] for entry in partner_pieces]
    total = sum(block.shape[0] for block in blocks)
    return pl.pallas_call(
        functools.partial(place_kernel, plan),
        out_shape=pltpu.VMEM((2, rows, columns), jnp.bfloat16),
        in_specs=[pl.BlockSpec(memory_space=pltpu.SMEM)]
        + [pl.BlockSpec(memory_space=pl.ANY) for _ in blocks],
        out_specs=pl.BlockSpec(memory_space=pltpu.VMEM),
        scratch_shapes=[pltpu.SemaphoreType.DMA((total,))],
        compiler_params=pltpu.CompilerParams(vmem_limit_bytes=1 << 20),
        name="place_weights",
    )(place, *blocks)


def layer_kernel(
    moment,
    info_ref,
    weight_ref,
    current_ref,
    own_ref,
    clean_ref,
    gain_ref,
    query_bias_ref,
    key_bias_ref,
    value_bias_ref,
    out_ref,
):
    rows, features = current_ref.shape
    section = info_ref[52]
    bucket = jnp.clip(moment - section, 0, 3)
    base = bucket * 13
    row = lax.broadcasted_iota(jnp.int32, (rows, HD), 0)
    lane = lax.broadcasted_iota(jnp.int32, (rows, HD), 1)
    begin = jnp.zeros((rows, HD), jnp.int32)
    hit = jnp.zeros((rows, HD), jnp.int32)
    start = jnp.int32(0)
    for k in range(4):
        length = info_ref[base + k]
        target = start + lax.rem(info_ref[base + 9 + k], length)
        target = jnp.where(info_ref[base + 5 + k] == section, target, -1)
        hit = hit + jnp.where(row == target, 1, 0)
        start = start + length
        begin = begin + jnp.where(row >= start, length, 0)
    position = (row - begin).astype(jnp.float32)
    exponent = jnp.where(lane < HD // 2, lane, lane - HD // 2).astype(jnp.float32)
    angles = position * jnp.exp(exponent * (-math.log(rope_base) / (HD // 2)))
    cosine = jnp.cos(angles)
    sinus = jnp.sin(angles)
    sinus = jnp.where(lane < HD // 2, -sinus, sinus)
    key_row = lax.broadcasted_iota(jnp.int32, (rows, rows), 1)
    query_row = lax.broadcasted_iota(jnp.int32, (rows, rows), 0)
    allowed = (key_row <= query_row) & (key_row >= begin[:, :rows])

    hidden = jnp.where(
        hit[:, 0:1] > 0,
        clean_ref[bucket].astype(jnp.float32),
        current_ref[...].astype(jnp.float32),
    )
    scale = lax.rsqrt(jnp.mean(hidden * hidden, axis=-1, keepdims=True) + epsilon)
    normed = (hidden * scale * gain_ref[...]).astype(jnp.bfloat16)

    def turned(heads):
        return (heads * cosine + pltpu.roll(heads, HD // 2, 1) * sinus).astype(jnp.bfloat16)

    queries_keys = jnp.dot(normed, weight_ref[0], preferred_element_type=jnp.float32)
    values_new = jnp.dot(normed, weight_ref[1, :, : KV * HD], preferred_element_type=jnp.float32)
    pieces = []
    per_group = HQ // KV
    for g in range(KV):
        at = features + g * HD
        keys = turned(queries_keys[:, at : at + HD] + key_bias_ref[:, g * HD : (g + 1) * HD])
        values = values_new[:, g * HD : (g + 1) * HD] + value_bias_ref[:, g * HD : (g + 1) * HD]
        values = values.astype(jnp.bfloat16)
        queries = []
        for h in range(g * per_group, (g + 1) * per_group):
            cols = slice(h * HD, (h + 1) * HD)
            queries.append(turned(queries_keys[:, cols] + query_bias_ref[:, cols]))
        queries = jnp.concatenate(queries, axis=0)
        scores = lax.dot_general(
            queries, keys, (((1,), (1,)), ((), ())), preferred_element_type=jnp.float32
        ) * HD ** (-0.5)
        scores = scores.reshape(per_group, rows, rows)
        scores = jnp.where(allowed[None], scores, -1e30)
        top = jnp.max(scores, axis=-1, keepdims=True)
        grown = jnp.exp(scores - top)
        weights = grown / jnp.sum(grown, axis=-1, keepdims=True)
        weights = weights.reshape(per_group * rows, rows).astype(jnp.bfloat16)
        mixed = jnp.dot(weights, values, preferred_element_type=jnp.float32).astype(jnp.bfloat16)
        pieces += [mixed[h * rows : (h + 1) * rows] for h in range(per_group)]
    attended = jnp.concatenate(pieces, axis=1)
    updated = hidden + jnp.dot(
        attended, weight_ref[1, :, KV * HD :], preferred_element_type=jnp.float32
    )

    @pl.when(section <= moment)
    def _():
        out_ref[...] = updated.astype(jnp.bfloat16)

    @pl.when(section > moment)
    def _():
        out_ref[...] = own_ref[...]


def layer(moment, info, weights, current, own, clean, gain, query_bias, key_bias, value_bias):
    vmem = pl.BlockSpec(memory_space=pltpu.VMEM)
    return pl.pallas_call(
        functools.partial(layer_kernel, moment),
        out_shape=jax.ShapeDtypeStruct(current.shape, current.dtype),
        in_specs=[pl.BlockSpec(memory_space=pltpu.SMEM)] + [vmem] * 8,
        out_specs=vmem,
        compiler_params=pltpu.CompilerParams(vmem_limit_bytes=16 << 20),
        name=f"layer_{moment}",
    )(info, weights, current, own, clean, gain, query_bias, key_bias, value_bias)


def rmsnorm(hidden, norm_gain):
    residual = hidden.astype(jnp.float32)
    scaled = residual * lax.rsqrt(jnp.mean(residual * residual, axis=-1, keepdims=True) + epsilon)
    return (scaled * norm_gain).astype(jnp.bfloat16)


def to_all(values):
    count = lax.axis_size(GROUP_SECTION)
    spread = jnp.broadcast_to(values[None], (count, values.shape[0]))
    return lax.all_to_all(spread, GROUP_SECTION, 0, 0, tiled=True)


def add_up(parts, axis):
    got = lax.all_to_all(parts, axis, 0, 0, tiled=True)
    return jnp.sum(got.astype(jnp.float32), axis=0).astype(jnp.bfloat16)


def answer_rows(answer_pairs, unembed, offset):
    count = lax.axis_size(GROUP)
    sections = lax.axis_size("section")
    prompts = answer_pairs.shape[1]
    pairs = answer_pairs.reshape(count, sections, prompts, 2).transpose(1, 0, 2, 3).reshape(-1, 2)
    vocab_ids = offset + jnp.arange(unembed.shape[0], dtype=jnp.int32)
    choosing = (pairs[:, 0:1] == vocab_ids[None, :]).astype(jnp.bfloat16) - (
        pairs[:, 1:2] == vocab_ids[None, :]
    ).astype(jnp.bfloat16)
    rows = jnp.dot(choosing, unembed, preferred_element_type=jnp.float32).astype(jnp.bfloat16)
    width = unembed.shape[1]
    rows = add_up(rows.reshape(sections, -1, width), "section")
    rows = add_up(rows.reshape(lax.axis_size("group_0"), -1, width), "group_0")
    return add_up(rows.reshape(-1, prompts, width), ("group_1", "group_2"))


def per_device(
    embed_in,
    clean_cache,
    lengths,
    patch_layer,
    patch_pos,
    answers,
    attn_gain,
    w_query,
    b_query,
    w_keyval,
    b_key,
    b_value,
    w_out,
    final_gain,
    unembed,
):
    sections = lax.axis_size("section")
    section = lax.axis_index("section")
    core = lax.axis_index("group_2")
    prompts = patch_layer.shape[1]
    features = embed_in.shape[2]
    own = embed_in[0]

    middle = w_keyval.shape[2] // 2
    half_0 = jnp.concatenate([w_query[0], w_keyval[0, :, :middle]], axis=1)
    half_1 = jnp.concatenate([w_keyval[0, :, middle:], w_out[0]], axis=1)
    kept = jnp.where(core == 0, half_0, half_1)
    got = swap_cores(jnp.where(core == 0, half_1, half_0))
    block = jnp.where(
        core == 0,
        jnp.concatenate([kept, got], axis=0),
        jnp.concatenate([got, kept], axis=0),
    )
    own_pieces = gather_section(block)
    partner_pieces = [(*entry[:3], swap_cores(entry[3])) for entry in own_pieces]
    place = jnp.stack([lax.axis_index("group_0"), lax.axis_index("group_1"), core]).astype(jnp.int32)
    weights = placed(own_pieces, partner_pieces, place, features, half_0.shape[1])

    known = to_all(
        jnp.concatenate([lengths[0], patch_layer[0], patch_pos[0], answers[0].reshape(-1)])
    )
    line = lax.dynamic_slice_in_dim(known, lax.axis_index(GROUP) * sections, sections, 0)[:, :13]
    info = jnp.concatenate([line.reshape(-1), section[None].astype(jnp.int32)])
    offset = lax.axis_index(GROUP_SECTION) * unembed.shape[0]
    rows_wanted = answer_rows(known[:, 13:21].reshape(-1, prompts, 2), unembed, offset)

    current = own
    finals = []
    routes = [
        [(0, 1), (1, 0)],
        [(0, 1), (1, 2), (2, 0)],
        [(0, 1), (1, 2), (2, 3), (3, 0)],
        [(0, 1), (1, 2), (2, 3), (3, 0)],
        [(1, 2), (2, 3), (3, 1)],
        [(2, 3), (3, 2)],
    ]
    for moment in range(2 * sections - 1):
        result = layer(
            moment,
            info,
            weights,
            current,
            own,
            clean_cache[0],
            attn_gain,
            b_query,
            b_key,
            b_value,
        )
        if moment < len(routes):
            current = lax.ppermute(result, "section", routes[moment])
            finals.append(current)
    own_rows = jnp.where(
        section == 0,
        finals[3],
        jnp.where(section == 1, finals[4], jnp.where(section == 2, finals[5], result)),
    )

    own_lengths = lengths[0]
    own_starts = jnp.cumsum(own_lengths) - own_lengths
    last_rows = own_starts[:prompts] + own_lengths[:prompts] - 1
    readout = rmsnorm(own_rows[last_rows], final_gain)
    own_diff = jnp.sum(readout.astype(jnp.float32) * rows_wanted.astype(jnp.float32), axis=-1)
    all_diffs = to_all(own_diff)
    distance = known[:, :prompts] - 1 - known[:, 9 : 9 + prompts] % known[:, :prompts]
    cell_ids = known[:, 5 : 5 + prompts] * MAXLEN + distance
    cells = jnp.arange(sections * MAXLEN, dtype=jnp.int32)
    cell_totals = jnp.sum(
        jnp.where(cell_ids.reshape(-1)[:, None] == cells, all_diffs.reshape(-1)[:, None], 0.0),
        axis=0,
    )
    return (own_rows[None], own_diff.reshape(1, prompts), cell_totals.reshape(sections, MAXLEN))


def solution(mesh):
    torus = Mesh(
        mesh.devices.reshape(8, 4, 2, mesh.shape["section"]),
        ("group_0", "group_1", "group_2", "section"),
    )
    in_specs = (
        P(GROUP_SECTION, None, None),
        P("section", GROUP, None, None),
        P(GROUP_SECTION, None),
        P(GROUP_SECTION, None),
        P(GROUP_SECTION, None),
        P(GROUP_SECTION, None, None),
        P("section", None),
        P("section", GROUP, None),
        P("section", None),
        P("section", GROUP, None),
        P("section", None),
        P("section", None),
        P("section", GROUP, None),
        P(),
        P(GROUP_SECTION, None),
    )
    out_specs = (P(GROUP_SECTION, None, None), P(GROUP_SECTION, None), P())
    return jax.shard_map(
        per_device, mesh=torus, in_specs=in_specs, out_specs=out_specs, check_vma=False
    )
```
